32 devices in a mesh: batch: 4 (over y, core), expert: 2 (over x), tensor: 4 (over z).
Axes of the slice: x: 2, y: 2, z: 4, core: 2. Of those that a mesh axis runs over, the one named last changes fastest.
Arguments:
- tokens: bfloat16 [2, 1024, 4096], P('expert', 'batch', 'tensor'), may hold values from -8 to 8
- gain: bfloat16 [4096], P('tensor'), may hold values from 0.5 to 1.5
- phi: bfloat16 [4096, 128], P('tensor'), may hold values from -1 to 1
- w_gate: bfloat16 [2, 4096, 14336], P('expert', None, ('batch', 'tensor')), may hold values from -0.125 to 0.125
- w_up: bfloat16 [2, 4096, 14336], P('expert', None, ('batch', 'tensor')), may hold values from -0.125 to 0.125
- w_down: bfloat16 [2, 14336, 4096], P('expert', ('batch', 'tensor')), may hold values from -0.09375 to 0.09375
Outputs:
- moe_out: bfloat16 [2, 1024, 4096], P('expert', 'batch', 'tensor')
The draws below stay inside these ranges and needn't reach their ends.
All inputs are finite; a program needn't handle non-finite values.
Results may differ from the reference program's by a relative error of at most 0.025.
Values may be sent and summed in bfloat16 or wider, within the bound.
No kernel may reach another device: no remote copies, remote signals or barrier semaphores. Data moves between devices by JAX's collectives and lax.ppermute only.
A program may use at most 128 MiB of HBM per device.

```python
import math
import jax
import jax.numpy as jnp
from jax import lax

D = 4096
FF = 14336
P_SIZE = 64
E = 2
GROUPS = 2
GROUP_TOK = 1024
SHARDS = 16


def draw_tokens(key, part):
    base_key = jax.random.fold_in(key, 21)
    values = jax.random.normal(base_key, (GROUPS, GROUP_TOK, D), jnp.float32)
    return jnp.clip(values, -8.0, 8.0).astype(jnp.bfloat16)


def draw_phi(key, part):
    base_draw = jax.random.normal(jax.random.fold_in(key, 31), (D, E * P_SIZE), jnp.float32) * (3.0 / math.sqrt(D))
    base_draw = jnp.clip(base_draw, -1.0, 1.0)
    return base_draw.astype(jnp.bfloat16)


def spiked(values, rng, source, target, parts, factor):
    owner, partner = [(jnp.arange(values.shape[position]) // (values.shape[position] // parts)).reshape([-1 if axis == position else 1 for axis in range(values.ndim)]) for position in (source, target)]
    chosen = jax.random.permutation(rng, parts)[partner]
    strong = (owner == chosen) | (owner == (partner + parts // 2) % parts)
    return jnp.where(strong, factor * values, values)


def steps_of(own_key, dims, cuts, least, top_value):
    factor_of = 1.0
    for position, blocks in cuts:
        heights = jax.random.uniform(jax.random.fold_in(jax.random.fold_in(own_key, 6), position), (blocks,), jnp.float32, least / len(cuts), top_value / len(cuts))
        factor_of = factor_of * jnp.repeat(jnp.exp(heights), dims[position] // blocks).reshape((-1,) + (1,) * (len(dims) - 1 - position))
    return factor_of


def noise(key, shape, deviation, most, split=(), kind=jnp.bfloat16):
    drawn = deviation * jax.random.normal(key, shape, jnp.float32)
    if split:
        drawn = drawn * steps_of(key, shape, split, -0.22, 0.18)
    return jnp.clip(drawn, -most, most).astype(kind)


def gaussian_with(own_key, shape, width, bound, shards, heavy, kind=jnp.bfloat16):
    values = width * jax.random.normal(own_key, shape, jnp.float32)
    if shards:
        values = values * steps_of(own_key, shape, shards, -0.22, 0.18)
    return jnp.clip(spiked(values, jax.random.fold_in(own_key, 3), *heavy), -bound, bound).astype(kind)


def setup_inputs(seed: int = 0) -> dict:
    splits = jax.random.split(jax.random.key(seed), 7)
    return {
        "tokens": draw_tokens(jax.random.fold_in(splits[6], 71), 0),
        "gain": jnp.clip(1.0 + 0.1 * jax.random.normal(splits[1], (D,), jnp.float32), 0.5, 1.5).astype(jnp.bfloat16),
        "phi": draw_phi(jax.random.fold_in(splits[6], 71), 0),
        "w_gate": noise(splits[3], (E, D, FF), (D // 2) ** -0.5, 0.125, ((0, 2), (2, 16))),
        "w_up": noise(splits[4], (E, D, FF), (D // 2) ** -0.5, 0.125, ((0, 2), (2, 16))),
        "w_down": gaussian_with(splits[5], (E, FF, D), (FF // 2) ** -0.5, 0.09375, ((0, 2), (1, 16)), (1, 2, 16, 2.0)),
    }


def reference(tokens, gain, phi, w_gate, w_up, w_down):
    tokens_f = tokens.astype(jnp.float32)
    gain_f = gain.astype(jnp.float32)
    scaled = (tokens_f * gain_f).astype(jnp.bfloat16)
    inv_rms = lax.rsqrt(lax.optimization_barrier(jnp.mean(tokens_f * tokens_f, axis=2)) + 1e-06)
    logits = jnp.einsum('gnd,ds->gns', scaled.astype(jnp.float32), phi.astype(jnp.float32)) * inv_rms[:, :, None]
    normed = (tokens_f * gain_f * inv_rms[:, :, None]).astype(jnp.bfloat16)
    column_max = lax.optimization_barrier(jnp.max(logits, axis=1, keepdims=True))
    raised = jnp.exp(logits - column_max)
    dispatch = (raised / lax.optimization_barrier(jnp.sum(raised, axis=1, keepdims=True))).astype(jnp.bfloat16)
    combine = jax.nn.softmax(logits, axis=2).astype(jnp.bfloat16)
    slot_in = jnp.einsum('gns,gnd->gsd', dispatch.astype(jnp.float32), normed.astype(jnp.float32)).astype(jnp.bfloat16)
    per_expert = slot_in.reshape(GROUPS, E, P_SIZE, D).transpose(1, 0, 2, 3).reshape(E, GROUPS * P_SIZE, D)

    def run_expert(expert_items):
        slot_rows, gate_weight, up_weight, down_weight = expert_items
        gate_act = jnp.dot(slot_rows, gate_weight, preferred_element_type=jnp.float32)
        up_act = jnp.dot(slot_rows, up_weight, preferred_element_type=jnp.float32)
        hidden = (jax.nn.silu(gate_act) * up_act).astype(jnp.bfloat16)
        block_width = FF // SHARDS
        pieces = hidden.reshape(GROUPS * P_SIZE, SHARDS, block_width).transpose(1, 0, 2).astype(jnp.float32)
        weights = down_weight.reshape(SHARDS, block_width, D).astype(jnp.float32)
        partials = jnp.einsum('krf,kfd->krd', pieces, weights).astype(jnp.bfloat16)
        partials = lax.optimization_barrier(partials)
        return lax.optimization_barrier(jnp.sum(partials.astype(jnp.float32), axis=0)).astype(jnp.bfloat16)
    slot_out = lax.map(run_expert, (per_expert, w_gate, w_up, w_down))
    slot_out = slot_out.reshape(E, GROUPS, P_SIZE, D).transpose(1, 0, 2, 3).reshape(GROUPS, E * P_SIZE, D)
    moe_out = jnp.einsum('gns,gsd->gnd', combine.astype(jnp.float32), slot_out.astype(jnp.float32))
    return moe_out.astype(jnp.bfloat16)
```

```python
import functools

import jax
import jax.numpy as jnp
from jax import lax
from jax.experimental import pallas as pl
from jax.experimental.pallas import tpu as pltpu
from jax.sharding import PartitionSpec as P

BF16, F32 = jnp.bfloat16, jnp.float32
VMEM = pl.BlockSpec(memory_space=pltpu.VMEM)
SMEM = pl.BlockSpec(memory_space=pltpu.SMEM)


def call(body, shapes, *args, cost=(1 << 30, 1 << 22), name=None):
    specs = [SMEM if a.dtype == jnp.int32 else VMEM for a in args]
    return pl.pallas_call(
        body,
        out_shape=shapes,
        in_specs=specs,
        out_specs=jax.tree.map(lambda _: VMEM, shapes),
        cost_estimate=pl.CostEstimate(flops=cost[0], bytes_accessed=cost[1], transcendentals=0),
        compiler_params=pltpu.CompilerParams(vmem_limit_bytes=24 << 20),
        name=name,
    )(*args)


def shape(dims, dtype):
    return jax.ShapeDtypeStruct(tuple(dims), dtype)


def swap(x, axes, bit):
    count = lax.axis_size(axes)
    return lax.ppermute(x, axes, [(i, i ^ bit) for i in range(count)])


def logits_body(tok_ref, gain_ref, phi_ref, scaled_ref, part_ref):
    tok = tok_ref[...].astype(F32)
    scaled = (tok * gain_ref[...].astype(F32)).astype(BF16)
    scaled_ref[...] = scaled
    slots = phi_ref.shape[1]
    part = jnp.dot(scaled, phi_ref[...], preferred_element_type=F32)
    part_ref[:slots] = part.T
    squares = jnp.sum(tok * tok, axis=1, keepdims=True)
    part_ref[slots:] = jnp.broadcast_to(squares, (tok.shape[0], 128)).T[:8]


def logits_of(part_refs, width):
    total = part_refs[0][...]
    for ref in part_refs[1:]:
        total = total + ref[...]
    slots = total.shape[0] - 8
    inv_rms = lax.rsqrt(total[slots : slots + 1] / width + 1e-06)
    return total[:slots] * inv_rms, inv_rms


def slots_body(width, n, *refs):
    part_refs, scaled_ref, message_ref = refs[:n], refs[n], refs[n + 1]
    logits, inv_rms = logits_of(part_refs, width)
    top = jnp.max(logits, axis=1, keepdims=True)
    raised = jnp.exp(logits - top)
    total = jnp.sum(raised, axis=1, keepdims=True)
    weights = (raised * (inv_rms / total)).astype(BF16)
    pieces, rows, wide = message_ref.shape
    share = scaled_ref.shape[1]
    slot = jnp.dot(weights, scaled_ref[...], preferred_element_type=F32)
    message_ref[:, :, :share] = slot.astype(BF16).reshape(pieces, rows, share)
    mass = top + jnp.log(total)
    high = mass.astype(BF16)
    rest = mass - high.astype(F32)
    middle = rest.astype(BF16)
    low = (rest - middle.astype(F32)).astype(BF16)
    lane = lax.broadcasted_iota(jnp.int32, (logits.shape[0], wide - share), 1)
    stats = jnp.where(
        lane == 0,
        high.astype(F32),
        jnp.where(lane == 1, middle.astype(F32), jnp.where(lane == 2, low.astype(F32), 0.0)),
    )
    message_ref[:, :, share:] = stats.astype(BF16).reshape(pieces, rows, wide - share)


def combine_body(width, n, experts, batches, where_ref, *refs):
    part_refs, out_ref, held = refs[:n], refs[n], refs[n + 1]
    logits, _ = logits_of(part_refs, width)
    raised = jnp.exp(logits - jnp.max(logits, axis=0, keepdims=True))
    held[...] = raised / jnp.sum(raised, axis=0, keepdims=True)
    rows = logits.shape[0] // (experts * batches)
    blocks = []
    for r in range(batches):
        for h in range(experts):
            at = ((where_ref[1] ^ h) * batches + (where_ref[0] ^ r)) * rows
            blocks.append(held[pl.ds(pl.multiple_of(at, rows), rows)])
    out_ref[...] = jnp.concatenate(blocks, axis=0).T.astype(BF16)


def gather_body(groups, batches, where_ref, message_ref, out_ref):
    rows, share = message_ref.shape[1], out_ref.shape[1]
    for h in range(groups):
        first = (where_ref[1] ^ h) * batches
        pieces = [message_ref[first + b].astype(F32) for b in range(batches)]
        mass = [
            p[:, share : share + 1] + p[:, share + 1 : share + 2] + p[:, share + 2 : share + 3]
            for p in pieces
        ]
        top = functools.reduce(jnp.maximum, mass)
        raised = [jnp.exp(m - top) for m in mass]
        total = functools.reduce(jnp.add, raised)
        out = sum(p[:, :share] * (w / total) for p, w in zip(pieces, raised))
        out_ref[h * rows : (h + 1) * rows] = out.astype(BF16)


def gate_up_body(batches, where_ref, *refs):
    steps = pl.num_programs(0)
    count = len(refs) - 5
    pieces, (gate_ref, up_ref, out_ref, gate, up) = refs[:count], refs[count:]
    step = pl.program_id(0)
    for s in range(count // batches):

        @pl.when(step == s)
        def _():
            x = jnp.concatenate([pieces[s * batches + r][...] for r in range(batches)], axis=0)
            g = jnp.dot(x, gate_ref[0], preferred_element_type=F32)
            u = jnp.dot(x, up_ref[0], preferred_element_type=F32)
            gate[...] = g if s == 0 else gate[...] + g
            up[...] = u if s == 0 else up[...] + u

    @pl.when(step == steps - 1)
    def _():
        g = gate[...]
        out_ref[...] = (g / (1.0 + jnp.exp(-g)) * up[...]).astype(BF16)


def gate_up(where, pieces, w_gate, w_up, batches):
    share = pieces[0].shape[1]
    rows = pieces[0].shape[0] * batches
    hidden = w_gate.shape[2]
    full = pl.BlockSpec(pieces[0].shape, lambda s, w: (0, 0))
    weight = pl.BlockSpec((1, share, hidden), lambda s, w: (0, w[2] ^ s, 0))
    return pl.pallas_call(
        functools.partial(gate_up_body, batches),
        grid_spec=pltpu.PrefetchScalarGridSpec(
            num_scalar_prefetch=1,
            grid=(len(pieces) // batches,),
            in_specs=[full] * len(pieces) + [weight, weight],
            out_specs=pl.BlockSpec((rows, hidden), lambda s, w: (0, 0)),
            scratch_shapes=[pltpu.VMEM((rows, hidden), F32)] * 2,
        ),
        out_shape=shape((rows, hidden), BF16),
        cost_estimate=pl.CostEstimate(
            flops=4 * rows * hidden * w_gate.shape[1], bytes_accessed=4 * w_gate.size, transcendentals=0
        ),
        compiler_params=pltpu.CompilerParams(vmem_limit_bytes=32 << 20),
        name="gate_up",
    )(where, *pieces, w_gate, w_up)


def down_body(batches, where_ref, hidden_ref, down_ref, *out_refs):
    out = jnp.dot(hidden_ref[...], down_ref[0], preferred_element_type=F32).astype(BF16)
    rows = out.shape[0] // batches
    for r in range(batches):
        out_refs[r][...] = out[r * rows : (r + 1) * rows]


def down(where, hidden, w_down, s, share, batches):
    rows, depth = hidden.shape
    cut = 2
    block = share // cut
    each = rows // batches
    return pl.pallas_call(
        functools.partial(down_body, batches),
        grid_spec=pltpu.PrefetchScalarGridSpec(
            num_scalar_prefetch=1,
            grid=(cut,),
            in_specs=[
                pl.BlockSpec((rows, depth), lambda j, w: (0, 0)),
                pl.BlockSpec((1, depth, block), lambda j, w: (0, 0, (w[2] ^ s) * cut + j)),
            ],
            out_specs=[pl.BlockSpec((each, block), lambda j, w: (0, j))] * batches,
        ),
        out_shape=[shape((each, share), BF16)] * batches,
        cost_estimate=pl.CostEstimate(
            flops=2 * rows * depth * share, bytes_accessed=2 * depth * share, transcendentals=0
        ),
        compiler_params=pltpu.CompilerParams(vmem_limit_bytes=24 << 20),
        name="down",
    )(where, hidden, w_down)


def output_body(combine_ref, *refs):
    pieces, out_ref = refs[:-1], refs[-1]
    slots = jnp.concatenate([p[...] for p in pieces], axis=0)
    out_ref[...] = jnp.dot(combine_ref[...], slots, preferred_element_type=F32).astype(BF16)


def add(*xs):
    return functools.reduce(jnp.add, [x.astype(F32) for x in xs]).astype(BF16)


def local(tokens, gain, phi, w_gate, w_up, w_down):
    batches, experts, tensors = (lax.axis_size(a) for a in ("batch", "expert", "tensor"))
    for n in (batches, experts, tensors):
        assert n & (n - 1) == 0
    assert tokens.shape[0] == 1 and w_gate.shape[0] == 1
    where = jnp.stack([lax.axis_index(a) for a in ("batch", "expert", "tensor")]).astype(jnp.int32)
    width = w_gate.shape[1]
    count, share = tokens.shape[1:]
    slots = phi.shape[1]
    rows = slots // (experts * batches)

    scaled, part = call(
        logits_body,
        [shape((count, share), BF16), shape((slots + 8, count), F32)],
        tokens[0],
        gain[None],
        phi,
        name="logits",
    )
    parts = [part] + [swap(part, "tensor", s) for s in range(1, tensors)]
    message = call(
        functools.partial(slots_body, width, tensors),
        shape((experts * batches, rows, share + 128), BF16),
        *parts,
        scaled,
        name="slots",
    )
    combine = pl.pallas_call(
        functools.partial(combine_body, width, tensors, experts, batches),
        out_shape=shape((count, slots), BF16),
        in_specs=[SMEM] + [VMEM] * tensors,
        out_specs=VMEM,
        scratch_shapes=[pltpu.VMEM((slots, count), F32)],
        cost_estimate=pl.CostEstimate(flops=1 << 30, bytes_accessed=1 << 22, transcendentals=0),
        compiler_params=pltpu.CompilerParams(vmem_limit_bytes=24 << 20),
        name="combine",
    )(where, *parts)
    message = lax.all_to_all(message, ("expert", "batch"), split_axis=0, concat_axis=0, tiled=True)
    own = call(
        functools.partial(gather_body, experts, batches),
        shape((experts * rows, share), BF16),
        where,
        message,
        name="gather",
    )
    pieces = []
    for s in range(tensors):
        group = {0: own if s == 0 else swap(own, "tensor", s)}
        bit = batches >> 1
        while bit:
            group.update({r | bit: swap(group[r], "batch", bit) for r in list(group)})
            bit >>= 1
        pieces += [group[r] for r in range(batches)]
    hidden = gate_up(where, pieces, w_gate, w_up, batches)

    arrived = [[] for _ in range(experts)]
    for s in reversed(range(tensors)):
        partial = dict(enumerate(down(where, hidden, w_down, s, share, batches)))
        bit = 1
        while bit < batches:
            partial = {
                r: add(partial[r], swap(partial[r | bit], "batch", bit)) for r in partial if not r & bit
            }
            bit <<= 1
        for h in range(experts):
            piece = partial[0][h * rows : (h + 1) * rows]
            if h or s:
                piece = swap(piece, ("expert", "tensor"), h * tensors + s)
            arrived[h].append(piece)
    out = jnp.concatenate([add(*a) for a in arrived], axis=0)
    gathered = [out] + [swap(out, "batch", r) for r in range(1, batches)]
    return call(
        output_body, shape((count, share), BF16), combine, *gathered, name="output"
    )[None]


def solution(mesh):
    placed = (
        P("expert", "batch", "tensor"),
        P("tensor"),
        P("tensor", None),
        P("expert", None, ("batch", "tensor")),
        P("expert", None, ("batch", "tensor")),
        P("expert", ("batch", "tensor"), None),
    )
    return jax.shard_map(
        local, mesh=mesh, in_specs=placed, out_specs=P("expert", "batch", "tensor"), check_vma=False
    )
```

```python
import functools

import jax
import jax.numpy as jnp
from jax import lax
from jax.experimental import pallas as pl
from jax.experimental.pallas import tpu as pltpu
from jax.sharding import PartitionSpec as P


BF16, F32 = jnp.bfloat16, jnp.float32
VMEM = pl.BlockSpec(memory_space=pltpu.VMEM)
SMEM = pl.BlockSpec(memory_space=pltpu.SMEM)


def call(body, shapes, *args, cost=(1 << 30, 1 << 22)):
    specs = [SMEM if a.dtype == jnp.int32 else VMEM for a in args]
    return pl.pallas_call(
        body,
        out_shape=shapes,
        in_specs=specs,
        out_specs=jax.tree.map(lambda _: VMEM, shapes),
        cost_estimate=pl.CostEstimate(flops=cost[0], bytes_accessed=cost[1], transcendentals=0),
        compiler_params=pltpu.CompilerParams(vmem_limit_bytes=6 << 20),
    )(*args)


def shape(dims, dtype):
    return jax.ShapeDtypeStruct(tuple(dims), dtype)


def swap(x, axes, bit):
    count = lax.axis_size(axes)
    return lax.ppermute(x, axes, [(i, i ^ bit) for i in range(count)])


def logits_body(tok_hbm, gain_hbm, phi_hbm, scaled_ref, part_ref, tok_ref, gain_ref, phi_ref, sems):
    copies = [
        pltpu.make_async_copy(tok_hbm, tok_ref, sems.at[0]),
        pltpu.make_async_copy(phi_hbm, phi_ref, sems.at[1]),
        pltpu.make_async_copy(gain_hbm, gain_ref, sems.at[2]),
    ]
    for c in copies:
        c.start()
    for c in copies:
        c.wait()
    tok = tok_ref[0].astype(F32)
    scaled = (tok * gain_ref[...].astype(F32)).astype(BF16)
    scaled_ref[...] = scaled
    slots = phi_ref.shape[1]
    part = jnp.dot(scaled, phi_ref[...], preferred_element_type=F32)
    part_ref[:slots] = part.T
    squares = jnp.sum(tok * tok, axis=1, keepdims=True)
    part_ref[slots:] = jnp.broadcast_to(squares, (tok.shape[0], 128)).T[:8]


def logits_of(part_refs, width):
    total = part_refs[0][...]
    for ref in part_refs[1:]:
        total = total + ref[...]
    slots = total.shape[0] - 8
    inv_rms = lax.rsqrt(total[slots : slots + 1] / width + 1e-06)
    return total[:slots] * inv_rms, inv_rms


def slots_body(width, n, experts, batches, where_ref, *refs):
    part_refs, scaled_ref, message_refs, held = refs[:n], refs[n], refs[n + 1 : -1], refs[-1]
    logits, inv_rms = logits_of(part_refs, width)
    top = jnp.max(logits, axis=1, keepdims=True)
    raised = jnp.exp(logits - top)
    total = jnp.sum(raised, axis=1, keepdims=True)
    weights = (raised * (inv_rms / total)).astype(BF16)
    share = scaled_ref.shape[1]
    rows = held.shape[0] // (experts * batches)
    slot = jnp.dot(weights, scaled_ref[...], preferred_element_type=F32)
    held[:, :share] = slot.astype(BF16)
    mass = top + jnp.log(total)
    high = mass.astype(BF16).astype(F32)
    middle = (mass - high).astype(BF16).astype(F32)
    low = mass - high - middle
    lane = lax.broadcasted_iota(jnp.int32, (held.shape[0], held.shape[1] - share), 1)
    stats = jnp.where(
        lane == 0, high, jnp.where(lane == 1, middle, jnp.where(lane == 2, low, 0.0))
    )
    held[:, share:] = stats.astype(BF16)
    for h in range(experts):
        for r in range(batches):
            at = ((where_ref[1] ^ h) * batches + (where_ref[0] ^ r)) * rows
            message_refs[h * batches + r][...] = held[pl.ds(pl.multiple_of(at, rows), rows)]


def combine_body(width, n, experts, batches, where_ref, *refs):
    part_refs, out_ref, held = refs[:n], refs[n], refs[n + 1]
    logits, _ = logits_of(part_refs, width)
    raised = jnp.exp(logits - jnp.max(logits, axis=0, keepdims=True))
    held[...] = raised / jnp.sum(raised, axis=0, keepdims=True)
    rows = logits.shape[0] // (experts * batches)
    blocks = []
    for r in range(batches):
        for h in range(experts):
            at = ((where_ref[1] ^ h) * batches + (where_ref[0] ^ r)) * rows
            blocks.append(held[pl.ds(pl.multiple_of(at, rows), rows)])
    out_ref[...] = jnp.concatenate(blocks, axis=0).T.astype(BF16)


def gather_body(groups, batches, *refs):
    out_ref = refs[-1]
    rows, share = refs[0].shape[0], out_ref.shape[1]
    for h in range(groups):
        pieces = [refs[h * batches + r][...].astype(F32) for r in range(batches)]
        mass = [
            p[:, share : share + 1] + p[:, share + 1 : share + 2] + p[:, share + 2 : share + 3]
            for p in pieces
        ]
        top = functools.reduce(jnp.maximum, mass)
        raised = [jnp.exp(m - top) for m in mass]
        total = functools.reduce(jnp.add, raised)
        out = sum(p[:, :share] * (w / total) for p, w in zip(pieces, raised))
        out_ref[h * rows : (h + 1) * rows] = out.astype(BF16)


def gate_up_body(s, last, where_ref, *refs):
    low_ref, high_ref, gate_ref, up_ref = refs[:4]
    share = low_ref.shape[1]
    at = pl.ds(pl.multiple_of((where_ref[2] ^ s) * share, share), share)
    x = jnp.concatenate([low_ref[...], high_ref[...]], axis=0)
    g = jnp.dot(x, gate_ref[0, at], preferred_element_type=F32)
    u = jnp.dot(x, up_ref[0, at], preferred_element_type=F32)
    if len(refs) > (5 if last else 6):
        g, u = g + refs[4][...], u + refs[5][...]
    if last:
        refs[-1][...] = (g / (1.0 + jnp.exp(-g)) * u).astype(BF16)
    else:
        refs[-2][...] = g
        refs[-1][...] = u


def down_body(s, where_ref, hidden_ref, down_ref, keep_ref, send_ref):
    share = keep_ref.shape[1]
    at = pl.ds(pl.multiple_of((where_ref[2] ^ s) * share, share), share)
    out = jnp.dot(hidden_ref[...], down_ref[0, :, at], preferred_element_type=F32).astype(BF16)
    half = out.shape[0] // 2
    keep_ref[...] = out[:half]
    send_ref[...] = out[half:]


def output_body(combine_ref, *refs):
    pieces, out_ref = refs[:-1], refs[-1]
    slots = jnp.concatenate([p[...] for p in pieces], axis=0)
    out_ref[...] = jnp.dot(combine_ref[...], slots, preferred_element_type=F32).astype(BF16)


def fetch_body(*refs):
    count = (len(refs) - 1) // 2
    copies = [
        pltpu.make_async_copy(refs[i], refs[count + i], refs[-1].at[i]) for i in range(count)
    ]
    for c in copies:
        c.start()
    for c in copies:
        c.wait()


def fetch(*arrays):
    return pl.pallas_call(
        fetch_body,
        out_shape=[pltpu.VMEM(a.shape, a.dtype) for a in arrays],
        in_specs=[pl.BlockSpec(memory_space=pltpu.HBM)] * len(arrays),
        out_specs=[VMEM] * len(arrays),
        scratch_shapes=[pltpu.SemaphoreType.DMA((len(arrays),))],
        cost_estimate=pl.CostEstimate(flops=1 << 30, bytes_accessed=1 << 25, transcendentals=0),
        compiler_params=pltpu.CompilerParams(vmem_limit_bytes=1 << 20),
        name="fetch",
    )(*(pltpu.with_memory_space_constraint(a, pltpu.HBM) for a in arrays))


def add(*xs):
    return functools.reduce(jnp.add, [x.astype(F32) for x in xs]).astype(BF16)


def local(tokens, gain, phi, w_gate, w_up, w_down):
    batches, experts, tensors = (lax.axis_size(a) for a in ("batch", "expert", "tensor"))
    for n in (batches, experts, tensors):
        assert n & (n - 1) == 0
    assert tokens.shape[0] == 1 and w_gate.shape[0] == 1
    where = jnp.stack([lax.axis_index(a) for a in ("batch", "expert", "tensor")]).astype(jnp.int32)
    width = w_gate.shape[1]
    count, share = tokens.shape[1:]
    slots = phi.shape[1]
    rows = slots // (experts * batches)

    scaled, part = pl.pallas_call(
        logits_body,
        out_shape=[shape((count, share), BF16), shape((slots + 8, count), F32)],
        in_specs=[pl.BlockSpec(memory_space=pltpu.HBM)] * 3,
        out_specs=[VMEM, VMEM],
        scratch_shapes=[
            pltpu.VMEM(tokens.shape, BF16),
            pltpu.VMEM(gain.shape, BF16),
            pltpu.VMEM(phi.shape, BF16),
            pltpu.SemaphoreType.DMA((3,)),
        ],
        cost_estimate=pl.CostEstimate(flops=1 << 30, bytes_accessed=1 << 22, transcendentals=0),
        compiler_params=pltpu.CompilerParams(vmem_limit_bytes=6 << 20),
        name="logits",
    )(*(pltpu.with_memory_space_constraint(x, pltpu.HBM) for x in (tokens, gain, phi)))
    parts = [part] + [swap(part, "tensor", s) for s in range(1, tensors)]
    messages = pl.pallas_call(
        functools.partial(slots_body, width, tensors, experts, batches),
        out_shape=[shape((rows, share + 128), BF16)] * (experts * batches),
        in_specs=[SMEM] + [VMEM] * (tensors + 1),
        out_specs=[VMEM] * (experts * batches),
        scratch_shapes=[pltpu.VMEM((slots, share + 128), BF16)],
        cost_estimate=pl.CostEstimate(flops=1 << 30, bytes_accessed=1 << 22, transcendentals=0),
        compiler_params=pltpu.CompilerParams(vmem_limit_bytes=6 << 20),
        name="slots",
    )(where, *parts, scaled)
    combine = pl.pallas_call(
        functools.partial(combine_body, width, tensors, experts, batches),
        out_shape=shape((count, slots), BF16),
        in_specs=[SMEM] + [VMEM] * tensors,
        out_specs=VMEM,
        scratch_shapes=[pltpu.VMEM((slots, count), F32)],
        cost_estimate=pl.CostEstimate(flops=1 << 30, bytes_accessed=1 << 22, transcendentals=0),
        compiler_params=pltpu.CompilerParams(vmem_limit_bytes=6 << 20),
        name="combine",
    )(where, *parts)
    arrived = [
        m if i == 0 else swap(m, ("batch", "expert"), i % batches * experts + i // batches)
        for i, m in enumerate(messages)
    ]
    own = call(
        functools.partial(gather_body, experts, batches),
        shape((experts * rows, share), BF16),
        *arrived,
    )
    w_gate, w_up, w_down = fetch(w_gate, w_up, w_down)
    hidden_share = w_gate.shape[2]
    all_rows = batches * experts * rows
    carry = []
    for s in [0, *range(tensors - 1, 0, -1)]:
        piece = own if s == 0 else swap(own, "tensor", s)
        bit = batches >> 1
        while bit > 1:
            piece = jnp.concatenate([piece, swap(piece, "batch", bit)], axis=0)
            bit >>= 1
        last = s == min(1, tensors - 1)
        carry = call(
            functools.partial(gate_up_body, s, last),
            shape((all_rows, hidden_share), BF16)
            if last
            else [shape((all_rows, hidden_share), F32)] * 2,
            where,
            piece,
            swap(piece, "batch", 1),
            w_gate,
            w_up,
            *carry,
            cost=(4 * all_rows * hidden_share * share, 1 << 24),
        )
    arrived = []
    for s in reversed(range(tensors)):
        keep, send = call(
            functools.partial(down_body, s),
            [shape((all_rows // 2, share), BF16)] * 2,
            where,
            carry,
            w_down,
            cost=(2 * all_rows * hidden_share * share, 1 << 23),
        )
        total = add(keep, swap(send, "batch", 1))
        bit = 2
        while bit < batches:
            half = total.shape[0] // 2
            other = swap(total[half:], "batch", bit)
            total = add(total[:half], other)
            bit <<= 1
        arrived.append(swap(total, "tensor", s) if s else total)
    total = add(*arrived)
    pieces = [total[h * rows : (h + 1) * rows] for h in range(experts)]
    pieces = [p if h == 0 else swap(p, "expert", h) for h, p in enumerate(pieces)]
    out = jnp.concatenate(pieces, axis=0)
    gathered = [out] + [swap(out, "batch", r) for r in range(1, batches)]
    return call(output_body, shape((count, share), BF16), combine, *gathered)[None]


def solution(mesh):
    placed = (
        P("expert", "batch", "tensor"),
        P("tensor"),
        P("tensor", None),
        P("expert", None, ("batch", "tensor")),
        P("expert", None, ("batch", "tensor")),
        P("expert", ("batch", "tensor"), None),
    )
    return jax.shard_map(
        local, mesh=mesh, in_specs=placed, out_specs=P("expert", "batch", "tensor"), check_vma=False
    )
```

```python
import functools

import jax
import jax.numpy as jnp
from jax import lax
from jax.experimental import pallas as pl
from jax.experimental.pallas import tpu as pltpu
from jax.sharding import PartitionSpec as P


BF16, F32 = jnp.bfloat16, jnp.float32
HEAD = 53
VMEM = pl.BlockSpec(memory_space=pltpu.VMEM)
SMEM = pl.BlockSpec(memory_space=pltpu.SMEM)


def call(body, shapes, *args, cost=(1 << 30, 1 << 22)):
    specs = [SMEM if a.dtype == jnp.int32 else VMEM for a in args]
    return pl.pallas_call(
        body,
        out_shape=shapes,
        in_specs=specs,
        out_specs=jax.tree.map(lambda _: VMEM, shapes),
        cost_estimate=pl.CostEstimate(flops=cost[0], bytes_accessed=cost[1], transcendentals=0),
        compiler_params=pltpu.CompilerParams(vmem_limit_bytes=6 << 20),
    )(*args)


def shape(dims, dtype):
    return jax.ShapeDtypeStruct(tuple(dims), dtype)


def swap(x, axes, bit):
    count = lax.axis_size(axes)
    return lax.ppermute(x, axes, [(i, i ^ bit) for i in range(count)])


def logits_body(tok_hbm, gain_hbm, phi_hbm, scaled_ref, part_ref, head_ref, tok_ref, gain_ref, phi_ref, sems):
    copies = [
        pltpu.make_async_copy(tok_hbm, tok_ref, sems.at[0]),
        pltpu.make_async_copy(phi_hbm, phi_ref, sems.at[1]),
        pltpu.make_async_copy(gain_hbm, gain_ref, sems.at[2]),
    ]
    for c in copies:
        c.start()
    for c in copies:
        c.wait()
    tok = tok_ref[0].astype(F32)
    scaled = (tok * gain_ref[...].astype(F32)).astype(BF16)
    scaled_ref[...] = scaled
    part = jnp.dot(scaled, phi_ref[...], preferred_element_type=F32).T
    squares = jnp.sum(tok * tok, axis=1, keepdims=True)
    part_ref[:8] = jnp.broadcast_to(squares, (tok.shape[0], 128)).T[:8]
    part_ref[8:] = part
    head = head_ref.shape[0]
    head_ref[:8] = part_ref[:8]
    head_ref[8:] = part[: head - 8]


def logits_of(own_ref, near_ref, tail_ref, more_refs, width):
    head = more_refs[0].shape[0] if more_refs else own_ref.shape[0]
    total = own_ref[:head] + near_ref[:head]
    for ref in more_refs:
        total = total + ref[...]
    inv_rms = lax.rsqrt(total[:1] / width + 1e-06)
    logits = jnp.concatenate([total[8:], tail_ref[...]], axis=0) if more_refs else total[8:]
    return logits * inv_rms, inv_rms


def slots_body(width, n, experts, batches, where_ref, *refs):
    part_refs, scaled_ref, message_refs, held = refs[:n], refs[n], refs[n + 1 : -1], refs[-1]
    logits, inv_rms = logits_of(*part_refs[:3], part_refs[3:], width)
    top = jnp.max(logits, axis=1, keepdims=True)
    raised = jnp.exp(logits - top)
    total = jnp.sum(raised, axis=1, keepdims=True)
    weights = (raised * (inv_rms / total)).astype(BF16)
    share = scaled_ref.shape[1]
    rows = held.shape[0] // (experts * batches)
    slot = jnp.dot(weights, scaled_ref[...], preferred_element_type=F32)
    held[:, :share] = slot.astype(BF16)
    mass = top + jnp.log(total)
    high = mass.astype(BF16).astype(F32)
    middle = (mass - high).astype(BF16).astype(F32)
    low = mass - high - middle
    lane = lax.broadcasted_iota(jnp.int32, (held.shape[0], held.shape[1] - share), 1)
    stats = jnp.where(
        lane == 0, high, jnp.where(lane == 1, middle, jnp.where(lane == 2, low, 0.0))
    )
    held[:, share:] = stats.astype(BF16)
    for h in range(experts):
        for r in range(batches):
            at = ((where_ref[1] ^ h) * batches + (where_ref[0] ^ r)) * rows
            message_refs[h * batches + r][...] = held[pl.ds(pl.multiple_of(at, rows), rows)]


def slot_order(batches, experts):
    near = [(r, 0) for r in range(batches)]
    return near + [(r, h) for r in range(batches) for h in range(1, experts)]


def combine_body(width, n, experts, batches, where_ref, *refs):
    part_refs, out_ref, held = refs[:n], refs[n], refs[n + 1]
    logits, _ = logits_of(*part_refs[:3], part_refs[3:], width)
    raised = jnp.exp(logits - jnp.max(logits, axis=0, keepdims=True))
    held[...] = raised / jnp.sum(raised, axis=0, keepdims=True)
    rows = logits.shape[0] // (experts * batches)
    blocks = []
    for r, h in slot_order(batches, experts):
        at = ((where_ref[1] ^ h) * batches + (where_ref[0] ^ r)) * rows
        blocks.append(held[pl.ds(pl.multiple_of(at, rows), rows)])
    out_ref[...] = jnp.concatenate(blocks, axis=0).T.astype(BF16)


def gather_body(groups, batches, *refs):
    out_ref = refs[-1]
    rows, share = refs[0].shape[0], out_ref.shape[1]
    for h in range(groups):
        pieces = [refs[h * batches + r][...].astype(F32) for r in range(batches)]
        mass = [
            p[:, share : share + 1] + p[:, share + 1 : share + 2] + p[:, share + 2 : share + 3]
            for p in pieces
        ]
        top = functools.reduce(jnp.maximum, mass)
        raised = [jnp.exp(m - top) for m in mass]
        total = functools.reduce(jnp.add, raised)
        out = sum(p[:, :share] * (w / total) for p, w in zip(pieces, raised))
        out_ref[h * rows : (h + 1) * rows] = out.astype(BF16)


def gate_up_body(s, last, where_ref, *refs):
    low_ref, high_ref, gate_ref, up_ref = refs[:4]
    share = low_ref.shape[1]
    at = pl.ds(pl.multiple_of((where_ref[2] ^ s) * share, share), share)
    x = jnp.concatenate([low_ref[...], high_ref[...]], axis=0)
    g = jnp.dot(x, gate_ref[0, at], preferred_element_type=F32)
    u = jnp.dot(x, up_ref[0, at], preferred_element_type=F32)
    if len(refs) > (5 if last else 6):
        g, u = g + refs[4][...], u + refs[5][...]
    if last:
        refs[-1][...] = (g / (1.0 + jnp.exp(-g)) * u).astype(BF16)
    else:
        refs[-2][...] = g
        refs[-1][...] = u


def down_body(s, where_ref, hidden_ref, down_ref, keep_ref, send_ref):
    share = keep_ref.shape[1]
    at = pl.ds(pl.multiple_of((where_ref[2] ^ s) * share, share), share)
    out = jnp.dot(hidden_ref[...], down_ref[0, :, at], preferred_element_type=F32).astype(BF16)
    half = out.shape[0] // 2
    keep_ref[...] = out[:half]
    send_ref[...] = out[half:]


def output_body(combine_ref, *refs):
    pieces, out_ref = refs[:-1], refs[-1]
    slots = jnp.concatenate([p[...] for p in pieces], axis=0)
    out_ref[...] = jnp.dot(combine_ref[...], slots, preferred_element_type=F32).astype(BF16)


def fetch_body(*refs):
    count = (len(refs) - 1) // 2
    copies = [
        pltpu.make_async_copy(refs[i], refs[count + i], refs[-1].at[i]) for i in range(count)
    ]
    for c in copies:
        c.start()
    for c in copies:
        c.wait()


def fetch(*arrays):
    return pl.pallas_call(
        fetch_body,
        out_shape=[pltpu.VMEM(a.shape, a.dtype) for a in arrays],
        in_specs=[pl.BlockSpec(memory_space=pltpu.HBM)] * len(arrays),
        out_specs=[VMEM] * len(arrays),
        scratch_shapes=[pltpu.SemaphoreType.DMA((len(arrays),))],
        cost_estimate=pl.CostEstimate(flops=1 << 30, bytes_accessed=1 << 25, transcendentals=0),
        compiler_params=pltpu.CompilerParams(vmem_limit_bytes=1 << 20),
        name="fetch",
    )(*(pltpu.with_memory_space_constraint(a, pltpu.HBM) for a in arrays))


def add(*xs):
    return functools.reduce(jnp.add, [x.astype(F32) for x in xs]).astype(BF16)


def local(tokens, gain, phi, w_gate, w_up, w_down):
    batches, experts, tensors = (lax.axis_size(a) for a in ("batch", "expert", "tensor"))
    for n in (batches, experts, tensors):
        assert n & (n - 1) == 0
    assert tokens.shape[0] == 1 and w_gate.shape[0] == 1
    where = jnp.stack([lax.axis_index(a) for a in ("batch", "expert", "tensor")]).astype(jnp.int32)
    width = w_gate.shape[1]
    count, share = tokens.shape[1:]
    slots = phi.shape[1]
    rows = slots // (experts * batches)

    head = 8 * max(1, (slots + 8) * HEAD // 800)
    scaled, part, first = pl.pallas_call(
        logits_body,
        out_shape=[
            shape((count, share), BF16),
            shape((slots + 8, count), F32),
            shape((head, count), F32),
        ],
        in_specs=[pl.BlockSpec(memory_space=pltpu.HBM)] * 3,
        out_specs=[VMEM] * 3,
        scratch_shapes=[
            pltpu.VMEM(tokens.shape, BF16),
            pltpu.VMEM(gain.shape, BF16),
            pltpu.VMEM(phi.shape, BF16),
            pltpu.SemaphoreType.DMA((3,)),
        ],
        cost_estimate=pl.CostEstimate(flops=1 << 30, bytes_accessed=1 << 22, transcendentals=0),
        compiler_params=pltpu.CompilerParams(vmem_limit_bytes=6 << 20),
        name="logits",
    )(*(pltpu.with_memory_space_constraint(x, pltpu.HBM) for x in (tokens, gain, phi)))
    near = swap(part, "tensor", 1)
    tail = part[head:] + near[head:]
    bit = 2
    while bit < tensors:
        tail = tail + swap(tail, "tensor", bit)
        bit <<= 1
    parts = [part, near, tail] + [swap(first, "tensor", s) for s in range(2, tensors)]
    parts_count = len(parts)
    messages = pl.pallas_call(
        functools.partial(slots_body, width, parts_count, experts, batches),
        out_shape=[shape((rows, share + 128), BF16)] * (experts * batches),
        in_specs=[SMEM] + [VMEM] * (parts_count + 1),
        out_specs=[VMEM] * (experts * batches),
        scratch_shapes=[pltpu.VMEM((slots, share + 128), BF16)],
        cost_estimate=pl.CostEstimate(flops=1 << 30, bytes_accessed=1 << 22, transcendentals=0),
        compiler_params=pltpu.CompilerParams(vmem_limit_bytes=6 << 20),
        name="slots",
    )(where, *parts, scaled)
    combine = pl.pallas_call(
        functools.partial(combine_body, width, parts_count, experts, batches),
        out_shape=shape((count, slots), BF16),
        in_specs=[SMEM] + [VMEM] * parts_count,
        out_specs=VMEM,
        scratch_shapes=[pltpu.VMEM((slots, count), F32)],
        cost_estimate=pl.CostEstimate(flops=1 << 30, bytes_accessed=1 << 22, transcendentals=0),
        compiler_params=pltpu.CompilerParams(vmem_limit_bytes=6 << 20),
        name="combine",
    )(where, *parts)
    arrived = [
        m if i == 0 else swap(m, ("batch", "expert"), i % batches * experts + i // batches)
        for i, m in enumerate(messages)
    ]
    own = call(
        functools.partial(gather_body, experts, batches),
        shape((experts * rows, share), BF16),
        *arrived,
    )
    (w_gate,) = fetch(w_gate)
    (w_up,) = fetch(w_up)
    (w_down,) = fetch(w_down)
    hidden_share = w_gate.shape[2]
    all_rows = batches * experts * rows
    carry = []
    for s in [0, 1, *range(tensors - 1, 1, -1)][:tensors]:
        piece = own if s == 0 else swap(own, "tensor", s)
        bit = batches >> 1
        while bit > 1:
            if direct(batches, s):
                other = swap(own, ("batch", "tensor"), bit * tensors + s)
            else:
                other = swap(piece, "batch", bit)
            piece = jnp.concatenate([piece, other], axis=0)
            bit >>= 1
        last = s == min(2, tensors - 1)
        carry = call(
            functools.partial(gate_up_body, s, last),
            shape((all_rows, hidden_share), BF16)
            if last
            else [shape((all_rows, hidden_share), F32)] * 2,
            where,
            piece,
            swap(piece, "batch", 1),
            w_gate,
            w_up,
            *carry,
            cost=(4 * all_rows * hidden_share * share, 1 << 24),
        )
    arrived = []
    for s in reversed(range(tensors)):
        keep, send = call(
            functools.partial(down_body, s),
            [shape((all_rows // 2, share), BF16)] * 2,
            where,
            carry,
            w_down,
            cost=(2 * all_rows * hidden_share * share, 1 << 23),
        )
        total = add(keep, swap(send, "batch", 1))
        bit = 2
        while bit < batches:
            half = total.shape[0] // 2
            other = swap(total[half:], "batch", bit)
            total = add(total[:half], other)
            bit <<= 1
        arrived.append(swap(total, "tensor", s) if s else total)
    total = add(*arrived)
    groups = [total[:rows]]
    if experts > 1:
        pieces = [swap(total[h * rows : (h + 1) * rows], "expert", h) for h in range(1, experts)]
        groups.append(jnp.concatenate(pieces, axis=0))
    gathered = []
    for group in groups:
        gathered += [group] + [swap(group, "batch", r) for r in range(1, batches)]
    return call(output_body, shape((count, share), BF16), combine, *gathered)[None]


def direct(batches, s):
    return s == 1 and batches == 4


def solution(mesh):
    placed = (
        P("expert", "batch", "tensor"),
        P("tensor"),
        P("tensor", None),
        P("expert", None, ("batch", "tensor")),
        P("expert", None, ("batch", "tensor")),
        P("expert", ("batch", "tensor"), None),
    )
    return jax.shard_map(
        local, mesh=mesh, in_specs=placed, out_specs=P("expert", "batch", "tensor"), check_vma=False
    )
```

```python
import functools

import jax
import jax.numpy as jnp
from jax import lax
from jax.experimental import pallas as pl
from jax.experimental.pallas import tpu as pltpu
from jax.sharding import PartitionSpec as P


BF16, F32 = jnp.bfloat16, jnp.float32
HEAD = 53
VMEM = pl.BlockSpec(memory_space=pltpu.VMEM)
SMEM = pl.BlockSpec(memory_space=pltpu.SMEM)


def call(body, shapes, *args, cost=(1 << 30, 1 << 22)):
    specs = [SMEM if a.dtype == jnp.int32 else VMEM for a in args]
    return pl.pallas_call(
        body,
        out_shape=shapes,
        in_specs=specs,
        out_specs=jax.tree.map(lambda _: VMEM, shapes),
        cost_estimate=pl.CostEstimate(flops=cost[0], bytes_accessed=cost[1], transcendentals=0),
        compiler_params=pltpu.CompilerParams(vmem_limit_bytes=6 << 20),
    )(*args)


def shape(dims, dtype):
    return jax.ShapeDtypeStruct(tuple(dims), dtype)


def swap(x, axes, bit):
    count = lax.axis_size(axes)
    return lax.ppermute(x, axes, [(i, i ^ bit) for i in range(count)])


def logits_body(tok_hbm, gain_hbm, phi_hbm, scaled_ref, part_ref, head_ref, tok_ref, gain_ref, phi_ref, sems):
    copies = [
        pltpu.make_async_copy(tok_hbm, tok_ref, sems.at[0]),
        pltpu.make_async_copy(phi_hbm, phi_ref, sems.at[1]),
        pltpu.make_async_copy(gain_hbm, gain_ref, sems.at[2]),
    ]
    for c in copies:
        c.start()
    for c in copies:
        c.wait()
    tok = tok_ref[0].astype(F32)
    scaled = (tok * gain_ref[...].astype(F32)).astype(BF16)
    scaled_ref[...] = scaled
    part = jnp.dot(scaled, phi_ref[...], preferred_element_type=F32).T
    squares = jnp.sum(tok * tok, axis=1, keepdims=True)
    part_ref[:8] = jnp.broadcast_to(squares, (tok.shape[0], 128)).T[:8]
    part_ref[8:] = part
    head = head_ref.shape[0]
    head_ref[:8] = part_ref[:8]
    head_ref[8:] = part[: head - 8]


def logits_of(own_ref, near_ref, tail_ref, more_refs, width):
    head = more_refs[0].shape[0] if more_refs else own_ref.shape[0]
    total = own_ref[:head] + near_ref[:head]
    for ref in more_refs:
        total = total + ref[...]
    inv_rms = lax.rsqrt(total[:1] / width + 1e-06)
    logits = jnp.concatenate([total[8:], tail_ref[...]], axis=0) if more_refs else total[8:]
    return logits * inv_rms, inv_rms


def mass_of(piece, share):
    lanes = [piece[:, share + i : share + i + 1].astype(F32) for i in range(3)]
    return lanes[0] + lanes[1] + lanes[2]


def mass_lanes(mass, lanes):
    high = mass.astype(BF16).astype(F32)
    middle = (mass - high).astype(BF16).astype(F32)
    low = mass - high - middle
    lane = lax.broadcasted_iota(jnp.int32, (mass.shape[0], lanes), 1)
    stats = jnp.where(
        lane == 0, high, jnp.where(lane == 1, middle, jnp.where(lane == 2, low, 0.0))
    )
    return stats.astype(BF16)


def slots_body(width, n, experts, batches, where_ref, *refs):
    part_refs, scaled_ref, keep_ref, send_ref, held = refs[:n], refs[n], *refs[n + 1 :]
    logits, inv_rms = logits_of(*part_refs[:3], part_refs[3:], width)
    top = jnp.max(logits, axis=1, keepdims=True)
    raised = jnp.exp(logits - top)
    total = jnp.sum(raised, axis=1, keepdims=True)
    weights = (raised * (inv_rms / total)).astype(BF16)
    share = scaled_ref.shape[1]
    rows = held.shape[0] // (experts * batches)
    slot = jnp.dot(weights, scaled_ref[...], preferred_element_type=F32)
    held[:, :share] = slot.astype(BF16)
    held[:, share:] = mass_lanes(top + jnp.log(total), held.shape[1] - share)
    for h in range(experts):
        for r in range(batches):
            at = ((where_ref[1] ^ h) * batches + (where_ref[0] ^ r)) * rows
            to = (h * (batches // 2) + r // 2) * rows
            target = send_ref if r % 2 else keep_ref
            target[to : to + rows] = held[pl.ds(pl.multiple_of(at, rows), rows)]


def merge_body(share, keep_ref, came_ref, *out_refs):
    one, two = keep_ref[...], came_ref[...]
    mass = [mass_of(p, share) for p in (one, two)]
    top = jnp.maximum(*mass)
    raised = [jnp.exp(m - top) for m in mass]
    total = raised[0] + raised[1]
    both = one[:, :share].astype(F32) * (raised[0] / total)
    both = (both + two[:, :share].astype(F32) * (raised[1] / total)).astype(BF16)
    lanes = mass_lanes(top + jnp.log(total), one.shape[1] - share)
    rows = out_refs[0].shape[0]
    for i, ref in enumerate(out_refs):
        ref[:, :share] = both[i * rows : (i + 1) * rows]
        ref[:, share:] = lanes[i * rows : (i + 1) * rows]


def slot_order(batches, experts):
    near = [(r, 0) for r in range(batches)]
    return near + [(r, h) for r in range(batches) for h in range(1, experts)]


def combine_body(width, n, experts, batches, where_ref, *refs):
    part_refs, out_ref, held = refs[:n], refs[n], refs[n + 1]
    logits, _ = logits_of(*part_refs[:3], part_refs[3:], width)
    raised = jnp.exp(logits - jnp.max(logits, axis=0, keepdims=True))
    held[...] = raised / jnp.sum(raised, axis=0, keepdims=True)
    rows = logits.shape[0] // (experts * batches)
    blocks = []
    for r, h in slot_order(batches, experts):
        at = ((where_ref[1] ^ h) * batches + (where_ref[0] ^ r)) * rows
        blocks.append(held[pl.ds(pl.multiple_of(at, rows), rows)])
    out_ref[...] = jnp.concatenate(blocks, axis=0).T.astype(BF16)


def gather_body(groups, count, *refs):
    out_ref = refs[-1]
    rows, share = refs[0].shape[0], out_ref.shape[1]
    for h in range(groups):
        pieces = [refs[h * count + i][...] for i in range(count)]
        mass = [mass_of(p, share) for p in pieces]
        top = functools.reduce(jnp.maximum, mass)
        raised = [jnp.exp(m - top) for m in mass]
        total = functools.reduce(jnp.add, raised)
        out = sum(p[:, :share].astype(F32) * (w / total) for p, w in zip(pieces, raised))
        out_ref[h * rows : (h + 1) * rows] = out.astype(BF16)


def gate_up_body(s, last, where_ref, *refs):
    low_ref, high_ref, gate_ref, up_ref = refs[:4]
    share = low_ref.shape[1]
    at = pl.ds(pl.multiple_of((where_ref[2] ^ s) * share, share), share)
    x = jnp.concatenate([low_ref[...], high_ref[...]], axis=0)
    g = jnp.dot(x, gate_ref[0, at], preferred_element_type=F32)
    u = jnp.dot(x, up_ref[0, at], preferred_element_type=F32)
    if len(refs) > (5 if last else 6):
        g, u = g + refs[4][...], u + refs[5][...]
    if last:
        refs[-1][...] = (g / (1.0 + jnp.exp(-g)) * u).astype(BF16)
    else:
        refs[-2][...] = g
        refs[-1][...] = u


def down_body(s, where_ref, hidden_ref, down_ref, keep_ref, send_ref):
    share = keep_ref.shape[1]
    at = pl.ds(pl.multiple_of((where_ref[2] ^ s) * share, share), share)
    out = jnp.dot(hidden_ref[...], down_ref[0, :, at], preferred_element_type=F32).astype(BF16)
    half = out.shape[0] // 2
    keep_ref[...] = out[:half]
    send_ref[...] = out[half:]


def output_body(combine_ref, *refs):
    pieces, out_ref = refs[:-1], refs[-1]
    slots = jnp.concatenate([p[...] for p in pieces], axis=0)
    out_ref[...] = jnp.dot(combine_ref[...], slots, preferred_element_type=F32).astype(BF16)


def fetch_body(*refs):
    count = (len(refs) - 1) // 2
    copies = [
        pltpu.make_async_copy(refs[i], refs[count + i], refs[-1].at[i]) for i in range(count)
    ]
    for c in copies:
        c.start()
    for c in copies:
        c.wait()


def fetch(*arrays):
    return pl.pallas_call(
        fetch_body,
        out_shape=[pltpu.VMEM(a.shape, a.dtype) for a in arrays],
        in_specs=[pl.BlockSpec(memory_space=pltpu.HBM)] * len(arrays),
        out_specs=[VMEM] * len(arrays),
        scratch_shapes=[pltpu.SemaphoreType.DMA((len(arrays),))],
        cost_estimate=pl.CostEstimate(flops=1 << 30, bytes_accessed=1 << 25, transcendentals=0),
        compiler_params=pltpu.CompilerParams(vmem_limit_bytes=1 << 20),
        name="fetch",
    )(*(pltpu.with_memory_space_constraint(a, pltpu.HBM) for a in arrays))


def add(*xs):
    return functools.reduce(jnp.add, [x.astype(F32) for x in xs]).astype(BF16)


def local(tokens, gain, phi, w_gate, w_up, w_down):
    batches, experts, tensors = (lax.axis_size(a) for a in ("batch", "expert", "tensor"))
    for n in (batches, experts, tensors):
        assert n & (n - 1) == 0
    assert tokens.shape[0] == 1 and w_gate.shape[0] == 1
    where = jnp.stack([lax.axis_index(a) for a in ("batch", "expert", "tensor")]).astype(jnp.int32)
    width = w_gate.shape[1]
    token_count, share = tokens.shape[1:]
    slots = phi.shape[1]
    rows = slots // (experts * batches)

    head = 8 * max(1, (slots + 8) * HEAD // 800)
    scaled, part, first = pl.pallas_call(
        logits_body,
        out_shape=[
            shape((token_count, share), BF16),
            shape((slots + 8, token_count), F32),
            shape((head, token_count), F32),
        ],
        in_specs=[pl.BlockSpec(memory_space=pltpu.HBM)] * 3,
        out_specs=[VMEM] * 3,
        scratch_shapes=[
            pltpu.VMEM(tokens.shape, BF16),
            pltpu.VMEM(gain.shape, BF16),
            pltpu.VMEM(phi.shape, BF16),
            pltpu.SemaphoreType.DMA((3,)),
        ],
        cost_estimate=pl.CostEstimate(flops=1 << 30, bytes_accessed=1 << 22, transcendentals=0),
        compiler_params=pltpu.CompilerParams(vmem_limit_bytes=6 << 20),
        name="logits",
    )(*(pltpu.with_memory_space_constraint(x, pltpu.HBM) for x in (tokens, gain, phi)))
    near = swap(part, "tensor", 1)
    tail = part[head:] + near[head:]
    bit = 2
    while bit < tensors:
        tail = tail + swap(tail, "tensor", bit)
        bit <<= 1
    parts = [part, near, tail] + [swap(first, "tensor", s) for s in range(2, tensors)]
    parts_count = len(parts)
    half = experts * batches // 2
    keep, send = pl.pallas_call(
        functools.partial(slots_body, width, parts_count, experts, batches),
        out_shape=[shape((half * rows, share + 128), BF16)] * 2,
        in_specs=[SMEM] + [VMEM] * (parts_count + 1),
        out_specs=[VMEM] * 2,
        scratch_shapes=[pltpu.VMEM((slots, share + 128), BF16)],
        cost_estimate=pl.CostEstimate(flops=1 << 30, bytes_accessed=1 << 22, transcendentals=0),
        compiler_params=pltpu.CompilerParams(vmem_limit_bytes=6 << 20),
        name="slots",
    )(where, *parts, scaled)
    messages = call(
        functools.partial(merge_body, share),
        [shape((rows, share + 128), BF16)] * half,
        keep,
        swap(send, "batch", 1),
    )
    combine = pl.pallas_call(
        functools.partial(combine_body, width, parts_count, experts, batches),
        out_shape=shape((token_count, slots), BF16),
        in_specs=[SMEM] + [VMEM] * parts_count,
        out_specs=VMEM,
        scratch_shapes=[pltpu.VMEM((slots, token_count), F32)],
        cost_estimate=pl.CostEstimate(flops=1 << 30, bytes_accessed=1 << 22, transcendentals=0),
        compiler_params=pltpu.CompilerParams(vmem_limit_bytes=6 << 20),
        name="combine",
    )(where, *parts)
    count = batches // 2
    arrived = [
        m if i == 0 else swap(m, ("batch", "expert"), i % count * 2 * experts + i // count)
        for i, m in enumerate(messages)
    ]
    own = call(
        functools.partial(gather_body, experts, count),
        shape((experts * rows, share), BF16),
        *arrived,
    )
    (w_gate,) = fetch(w_gate)
    (w_up,) = fetch(w_up)
    (w_down,) = fetch(w_down)
    hidden_share = w_gate.shape[2]
    all_rows = batches * experts * rows
    carry = []
    for s in [0, 1, *range(tensors - 1, 1, -1)][:tensors]:
        piece = own if s == 0 else swap(own, "tensor", s)
        bit = batches >> 1
        while bit > 1:
            if direct(batches, s):
                other = swap(own, ("batch", "tensor"), bit * tensors + s)
            else:
                other = swap(piece, "batch", bit)
            piece = jnp.concatenate([piece, other], axis=0)
            bit >>= 1
        last = s == min(2, tensors - 1)
        carry = call(
            functools.partial(gate_up_body, s, last),
            shape((all_rows, hidden_share), BF16)
            if last
            else [shape((all_rows, hidden_share), F32)] * 2,
            where,
            piece,
            swap(piece, "batch", 1),
            w_gate,
            w_up,
            *carry,
            cost=(4 * all_rows * hidden_share * share, 1 << 24),
        )
    arrived = []
    for s in reversed(range(tensors)):
        keep, send = call(
            functools.partial(down_body, s),
            [shape((all_rows // 2, share), BF16)] * 2,
            where,
            carry,
            w_down,
            cost=(2 * all_rows * hidden_share * share, 1 << 23),
        )
        total = add(keep, swap(send, "batch", 1))
        bit = 2
        while bit < batches:
            half = total.shape[0] // 2
            other = swap(total[half:], "batch", bit)
            total = add(total[:half], other)
            bit <<= 1
        arrived.append(swap(total, "tensor", s) if s else total)
    total = add(*arrived)
    groups = [total[:rows]]
    if experts > 1:
        pieces = [swap(total[h * rows : (h + 1) * rows], "expert", h) for h in range(1, experts)]
        groups.append(jnp.concatenate(pieces, axis=0))
    gathered = []
    for group in groups:
        gathered += [group] + [swap(group, "batch", r) for r in range(1, batches)]
    return call(output_body, shape((token_count, share), BF16), combine, *gathered)[None]


def direct(batches, s):
    return s == 1 and batches == 4


def solution(mesh):
    placed = (
        P("expert", "batch", "tensor"),
        P("tensor"),
        P("tensor", None),
        P("expert", None, ("batch", "tensor")),
        P("expert", None, ("batch", "tensor")),
        P("expert", ("batch", "tensor"), None),
    )
    return jax.shard_map(
        local, mesh=mesh, in_specs=placed, out_specs=P("expert", "batch", "tensor"), check_vma=False
    )
```

```python
import functools

import jax
import jax.numpy as jnp
from jax import lax
from jax.experimental import pallas as pl
from jax.experimental.pallas import tpu as pltpu
from jax.sharding import PartitionSpec as P


BF16, F32 = jnp.bfloat16, jnp.float32
HEAD = 53
VMEM = pl.BlockSpec(memory_space=pltpu.VMEM)


def call(body, shapes, *args, cost=(1 << 30, 1 << 22)):
    return pl.pallas_call(
        body,
        out_shape=shapes,
        in_specs=[VMEM] * len(args),
        out_specs=jax.tree.map(lambda _: VMEM, shapes),
        cost_estimate=pl.CostEstimate(flops=cost[0], bytes_accessed=cost[1], transcendentals=0),
        compiler_params=pltpu.CompilerParams(vmem_limit_bytes=6 << 20),
    )(*args)


def shape(dims, dtype):
    return jax.ShapeDtypeStruct(tuple(dims), dtype)


def swap(x, axes, bit):
    count = lax.axis_size(axes)
    return lax.ppermute(x, axes, [(i, i ^ bit) for i in range(count)])


def logits_body(tok_hbm, gain_hbm, phi_hbm, scaled_ref, part_ref, head_ref, tok_ref, gain_ref, phi_ref, sems):
    copies = [
        pltpu.make_async_copy(tok_hbm, tok_ref, sems.at[0]),
        pltpu.make_async_copy(phi_hbm, phi_ref, sems.at[1]),
        pltpu.make_async_copy(gain_hbm, gain_ref, sems.at[2]),
    ]
    for c in copies:
        c.start()
    for c in copies:
        c.wait()
    tok = tok_ref[0].astype(F32)
    scaled = (tok * gain_ref[...].astype(F32)).astype(BF16)
    scaled_ref[...] = scaled
    part = jnp.dot(scaled, phi_ref[...], preferred_element_type=F32).T
    squares = jnp.sum(tok * tok, axis=1, keepdims=True)
    part_ref[:8] = jnp.broadcast_to(squares, (tok.shape[0], 128)).T[:8]
    part_ref[8:] = part
    head = head_ref.shape[0]
    head_ref[:8] = part_ref[:8]
    head_ref[8:] = part[: head - 8]


def logits_of(own_ref, near_ref, tail_ref, more_refs, width):
    head = more_refs[0].shape[0] if more_refs else own_ref.shape[0]
    total = own_ref[:head] + near_ref[:head]
    for ref in more_refs:
        total = total + ref[...]
    inv_rms = lax.rsqrt(total[:1] / width + 1e-06)
    logits = jnp.concatenate([total[8:], tail_ref[...]], axis=0) if more_refs else total[8:]
    return logits * inv_rms, inv_rms


def mass_of(piece, share):
    lanes = [piece[:, share + i : share + i + 1].astype(F32) for i in range(3)]
    return lanes[0] + lanes[1] + lanes[2]


def mass_lanes(mass, lanes):
    high = mass.astype(BF16).astype(F32)
    middle = (mass - high).astype(BF16).astype(F32)
    low = mass - high - middle
    lane = lax.broadcasted_iota(jnp.int32, (mass.shape[0], lanes), 1)
    stats = jnp.where(
        lane == 0, high, jnp.where(lane == 1, middle, jnp.where(lane == 2, low, 0.0))
    )
    return stats.astype(BF16)


def slots_body(width, n, experts, batches, *refs):
    part_refs, scaled_ref, keep_ref, send_ref, held = refs[:n], refs[n], *refs[n + 1 :]
    logits, inv_rms = logits_of(*part_refs[:3], part_refs[3:], width)
    top = jnp.max(logits, axis=1, keepdims=True)
    raised = jnp.exp(logits - top)
    total = jnp.sum(raised, axis=1, keepdims=True)
    weights = (raised * (inv_rms / total)).astype(BF16)
    share = scaled_ref.shape[1]
    rows = held.shape[0] // (experts * batches)
    slot = jnp.dot(weights, scaled_ref[...], preferred_element_type=F32)
    held[:, :share] = slot.astype(BF16)
    held[:, share:] = mass_lanes(top + jnp.log(total), held.shape[1] - share)
    for h in range(experts):
        for r in range(batches):
            at = ((lax.axis_index("expert") ^ h) * batches + (lax.axis_index("batch") ^ r)) * rows
            to = (h * (batches // 2) + r // 2) * rows
            target = send_ref if r % 2 else keep_ref
            target[to : to + rows] = held[pl.ds(pl.multiple_of(at, rows), rows)]


def merge_body(share, keep_ref, came_ref, *out_refs):
    one, two = keep_ref[...], came_ref[...]
    mass = [mass_of(p, share) for p in (one, two)]
    top = jnp.maximum(*mass)
    raised = [jnp.exp(m - top) for m in mass]
    total = raised[0] + raised[1]
    both = one[:, :share].astype(F32) * (raised[0] / total)
    both = (both + two[:, :share].astype(F32) * (raised[1] / total)).astype(BF16)
    lanes = mass_lanes(top + jnp.log(total), one.shape[1] - share)
    rows = out_refs[0].shape[0]
    for i, ref in enumerate(out_refs):
        ref[:, :share] = both[i * rows : (i + 1) * rows]
        ref[:, share:] = lanes[i * rows : (i + 1) * rows]


def slot_order(batches, experts):
    near = [(r, 0) for r in range(batches)]
    return near + [(r, h) for r in range(batches) for h in range(1, experts)]


def combine_body(width, n, experts, batches, *refs):
    part_refs, out_ref, held = refs[:n], refs[n], refs[n + 1]
    logits, _ = logits_of(*part_refs[:3], part_refs[3:], width)
    raised = jnp.exp(logits - jnp.max(logits, axis=0, keepdims=True))
    held[...] = raised / jnp.sum(raised, axis=0, keepdims=True)
    rows = logits.shape[0] // (experts * batches)
    blocks = []
    for r, h in slot_order(batches, experts):
        at = ((lax.axis_index("expert") ^ h) * batches + (lax.axis_index("batch") ^ r)) * rows
        blocks.append(held[pl.ds(pl.multiple_of(at, rows), rows)])
    out_ref[...] = jnp.concatenate(blocks, axis=0).T.astype(BF16)


def gather_body(groups, count, *refs):
    out_ref = refs[-1]
    rows, share = refs[0].shape[0], out_ref.shape[1]
    for h in range(groups):
        pieces = [refs[h * count + i][...] for i in range(count)]
        mass = [mass_of(p, share) for p in pieces]
        top = functools.reduce(jnp.maximum, mass)
        raised = [jnp.exp(m - top) for m in mass]
        total = functools.reduce(jnp.add, raised)
        out = sum(p[:, :share].astype(F32) * (w / total) for p, w in zip(pieces, raised))
        out_ref[h * rows : (h + 1) * rows] = out.astype(BF16)


def gate_up_body(s, last, *refs):
    low_ref, high_ref, gate_ref, up_ref = refs[:4]
    share = low_ref.shape[1]
    at = pl.ds(pl.multiple_of((lax.axis_index("tensor") ^ s) * share, share), share)
    x = jnp.concatenate([low_ref[...], high_ref[...]], axis=0)
    g = jnp.dot(x, gate_ref[0, at], preferred_element_type=F32)
    u = jnp.dot(x, up_ref[0, at], preferred_element_type=F32)
    if len(refs) > (5 if last else 6):
        g, u = g + refs[4][...], u + refs[5][...]
    if last:
        refs[-1][...] = (g / (1.0 + jnp.exp(-g)) * u).astype(BF16)
    else:
        refs[-2][...] = g
        refs[-1][...] = u


def down_body(s, hidden_ref, down_ref, keep_ref, send_ref):
    share = keep_ref.shape[1]
    at = pl.ds(pl.multiple_of((lax.axis_index("tensor") ^ s) * share, share), share)
    out = jnp.dot(hidden_ref[...], down_ref[0, :, at], preferred_element_type=F32).astype(BF16)
    half = out.shape[0] // 2
    keep_ref[...] = out[:half]
    send_ref[...] = out[half:]


def output_body(combine_ref, *refs):
    pieces, out_ref = refs[:-1], refs[-1]
    slots = jnp.concatenate([p[...] for p in pieces], axis=0)
    out_ref[...] = jnp.dot(combine_ref[...], slots, preferred_element_type=F32).astype(BF16)


def fetch_body(*refs):
    count = (len(refs) - 1) // 2
    copies = [
        pltpu.make_async_copy(refs[i], refs[count + i], refs[-1].at[i]) for i in range(count)
    ]
    for c in copies:
        c.start()
    for c in copies:
        c.wait()


def fetch(*arrays):
    return pl.pallas_call(
        fetch_body,
        out_shape=[pltpu.VMEM(a.shape, a.dtype) for a in arrays],
        in_specs=[pl.BlockSpec(memory_space=pltpu.HBM)] * len(arrays),
        out_specs=[VMEM] * len(arrays),
        scratch_shapes=[pltpu.SemaphoreType.DMA((len(arrays),))],
        cost_estimate=pl.CostEstimate(flops=1 << 30, bytes_accessed=1 << 25, transcendentals=0),
        compiler_params=pltpu.CompilerParams(vmem_limit_bytes=1 << 20),
        name="fetch",
    )(*(pltpu.with_memory_space_constraint(a, pltpu.HBM) for a in arrays))


def add(*xs):
    return functools.reduce(jnp.add, [x.astype(F32) for x in xs]).astype(BF16)


def local(tokens, gain, phi, w_gate, w_up, w_down):
    batches, experts, tensors = (lax.axis_size(a) for a in ("batch", "expert", "tensor"))
    for n in (batches, experts, tensors):
        assert n & (n - 1) == 0
    assert tokens.shape[0] == 1 and w_gate.shape[0] == 1
    width = w_gate.shape[1]
    token_count, share = tokens.shape[1:]
    slots = phi.shape[1]
    rows = slots // (experts * batches)

    head = 8 * max(1, (slots + 8) * HEAD // 800)
    scaled, part, first = pl.pallas_call(
        logits_body,
        out_shape=[
            shape((token_count, share), BF16),
            shape((slots + 8, token_count), F32),
            shape((head, token_count), F32),
        ],
        in_specs=[pl.BlockSpec(memory_space=pltpu.HBM)] * 3,
        out_specs=[VMEM] * 3,
        scratch_shapes=[
            pltpu.VMEM(tokens.shape, BF16),
            pltpu.VMEM(gain.shape, BF16),
            pltpu.VMEM(phi.shape, BF16),
            pltpu.SemaphoreType.DMA((3,)),
        ],
        cost_estimate=pl.CostEstimate(flops=1 << 30, bytes_accessed=1 << 22, transcendentals=0),
        compiler_params=pltpu.CompilerParams(vmem_limit_bytes=6 << 20),
        name="logits",
    )(*(pltpu.with_memory_space_constraint(x, pltpu.HBM) for x in (tokens, gain, phi)))
    near = swap(part, "tensor", 1)
    tail = part[head:] + near[head:]
    bit = 2
    while bit < tensors:
        tail = tail + swap(tail, "tensor", bit)
        bit <<= 1
    parts = [part, near, tail] + [swap(first, "tensor", s) for s in range(2, tensors)]
    parts_count = len(parts)
    half = experts * batches // 2
    keep, send = pl.pallas_call(
        functools.partial(slots_body, width, parts_count, experts, batches),
        out_shape=[shape((half * rows, share + 128), BF16)] * 2,
        in_specs=[VMEM] * (parts_count + 1),
        out_specs=[VMEM] * 2,
        scratch_shapes=[pltpu.VMEM((slots, share + 128), BF16)],
        cost_estimate=pl.CostEstimate(flops=1 << 30, bytes_accessed=1 << 22, transcendentals=0),
        compiler_params=pltpu.CompilerParams(vmem_limit_bytes=6 << 20),
        name="slots",
    )(*parts, scaled)
    messages = call(
        functools.partial(merge_body, share),
        [shape((rows, share + 128), BF16)] * half,
        keep,
        swap(send, "batch", 1),
    )
    combine = pl.pallas_call(
        functools.partial(combine_body, width, parts_count, experts, batches),
        out_shape=shape((token_count, slots), BF16),
        in_specs=[VMEM] * parts_count,
        out_specs=VMEM,
        scratch_shapes=[pltpu.VMEM((slots, token_count), F32)],
        cost_estimate=pl.CostEstimate(flops=1 << 30, bytes_accessed=1 << 22, transcendentals=0),
        compiler_params=pltpu.CompilerParams(vmem_limit_bytes=6 << 20),
        name="combine",
    )(*parts)
    count = batches // 2
    arrived = [
        m if i == 0 else swap(m, ("batch", "expert"), i % count * 2 * experts + i // count)
        for i, m in enumerate(messages)
    ]
    own = call(
        functools.partial(gather_body, experts, count),
        shape((experts * rows, share), BF16),
        *arrived,
    )
    (w_gate,) = fetch(w_gate)
    (w_up,) = fetch(w_up)
    (w_down,) = fetch(w_down)
    hidden_share = w_gate.shape[2]
    all_rows = batches * experts * rows
    carry = []
    for s in [0, 1, *range(tensors - 1, 1, -1)][:tensors]:
        piece = own if s == 0 else swap(own, "tensor", s)
        bit = batches >> 1
        while bit > 1:
            if direct(batches, s):
                other = swap(own, ("batch", "tensor"), bit * tensors + s)
            else:
                other = swap(piece, "batch", bit)
            piece = jnp.concatenate([piece, other], axis=0)
            bit >>= 1
        last = s == min(2, tensors - 1)
        carry = call(
            functools.partial(gate_up_body, s, last),
            shape((all_rows, hidden_share), BF16)
            if last
            else [shape((all_rows, hidden_share), F32)] * 2,
            piece,
            swap(piece, "batch", 1),
            w_gate,
            w_up,
            *carry,
            cost=(4 * all_rows * hidden_share * share, 1 << 24),
        )
    arrived = []
    for s in reversed(range(tensors)):
        keep, send = call(
            functools.partial(down_body, s),
            [shape((all_rows // 2, share), BF16)] * 2,
                carry,
            w_down,
            cost=(2 * all_rows * hidden_share * share, 1 << 23),
        )
        total = add(keep, swap(send, "batch", 1))
        bit = 2
        while bit < batches:
            half = total.shape[0] // 2
            other = swap(total[half:], "batch", bit)
            total = add(total[:half], other)
            bit <<= 1
        arrived.append(swap(total, "tensor", s) if s else total)
    total = add(*arrived)
    groups = [total[:rows]]
    if experts > 1:
        pieces = [swap(total[h * rows : (h + 1) * rows], "expert", h) for h in range(1, experts)]
        groups.append(jnp.concatenate(pieces, axis=0))
    gathered = []
    for group in groups:
        gathered += [group] + [swap(group, "batch", r) for r in range(1, batches)]
    return call(output_body, shape((token_count, share), BF16), combine, *gathered)[None]


def direct(batches, s):
    return s == 1 and batches == 4


def solution(mesh):
    placed = (
        P("expert", "batch", "tensor"),
        P("tensor"),
        P("tensor", None),
        P("expert", None, ("batch", "tensor")),
        P("expert", None, ("batch", "tensor")),
        P("expert", ("batch", "tensor"), None),
    )
    return jax.shard_map(
        local, mesh=mesh, in_specs=placed, out_specs=P("expert", "batch", "tensor"), check_vma=False
    )
```

```python
import functools

import jax
import jax.numpy as jnp
from jax import lax
from jax.experimental import pallas as pl
from jax.experimental.pallas import tpu as pltpu
from jax.sharding import PartitionSpec as P


BF16, F32 = jnp.bfloat16, jnp.float32
HEAD = 53
VMEM = pl.BlockSpec(memory_space=pltpu.VMEM)


def call(body, shapes, *args, cost=(1 << 30, 1 << 22)):
    return pl.pallas_call(
        body,
        out_shape=shapes,
        in_specs=[VMEM] * len(args),
        out_specs=jax.tree.map(lambda _: VMEM, shapes),
        cost_estimate=pl.CostEstimate(flops=cost[0], bytes_accessed=cost[1], transcendentals=0),
        compiler_params=pltpu.CompilerParams(vmem_limit_bytes=6 << 20),
    )(*args)


def shape(dims, dtype):
    return jax.ShapeDtypeStruct(tuple(dims), dtype)


def swap(x, axes, bit):
    count = lax.axis_size(axes)
    return lax.ppermute(x, axes, [(i, i ^ bit) for i in range(count)])


def logits_body(tok_hbm, gain_hbm, phi_hbm, scaled_ref, part_ref, head_ref, tok_ref, gain_ref, phi_ref, sems):
    copies = [
        pltpu.make_async_copy(tok_hbm, tok_ref, sems.at[0]),
        pltpu.make_async_copy(phi_hbm, phi_ref, sems.at[1]),
        pltpu.make_async_copy(gain_hbm, gain_ref, sems.at[2]),
    ]
    for c in copies:
        c.start()
    for c in copies:
        c.wait()
    tok = tok_ref[0].astype(F32)
    scaled = (tok * gain_ref[...].astype(F32)).astype(BF16)
    scaled_ref[...] = scaled
    part = jnp.dot(scaled, phi_ref[...], preferred_element_type=F32).T
    squares = jnp.sum(tok * tok, axis=1, keepdims=True)
    part_ref[:8] = jnp.broadcast_to(squares, (tok.shape[0], 128)).T[:8]
    part_ref[8:] = part
    head = head_ref.shape[0]
    head_ref[:8] = part_ref[:8]
    head_ref[8:] = part[: head - 8]


def logits_of(own_ref, near_ref, tail_ref, more_refs, width):
    head = more_refs[0].shape[0] if more_refs else own_ref.shape[0]
    total = own_ref[:head] + near_ref[:head]
    for ref in more_refs:
        total = total + ref[...]
    inv_rms = lax.rsqrt(total[:1] / width + 1e-06)
    logits = jnp.concatenate([total[8:], tail_ref[...]], axis=0) if more_refs else total[8:]
    return logits * inv_rms, inv_rms


def mass_of(piece, share):
    lanes = [piece[:, share + i : share + i + 1].astype(F32) for i in range(3)]
    return lanes[0] + lanes[1] + lanes[2]


def mass_lanes(mass, lanes):
    high = mass.astype(BF16).astype(F32)
    middle = (mass - high).astype(BF16).astype(F32)
    low = mass - high - middle
    lane = lax.broadcasted_iota(jnp.int32, (mass.shape[0], lanes), 1)
    stats = jnp.where(
        lane == 0, high, jnp.where(lane == 1, middle, jnp.where(lane == 2, low, 0.0))
    )
    return stats.astype(BF16)


def slots_body(width, n, experts, batches, *refs):
    part_refs, scaled_ref, keep_ref, send_ref, held = refs[:n], refs[n], *refs[n + 1 :]
    logits, inv_rms = logits_of(*part_refs[:3], part_refs[3:], width)
    top = jnp.max(logits, axis=1, keepdims=True)
    raised = jnp.exp(logits - top)
    total = jnp.sum(raised, axis=1, keepdims=True)
    weights = (raised * (inv_rms / total)).astype(BF16)
    share = scaled_ref.shape[1]
    rows = held.shape[0] // (experts * batches)
    slot = jnp.dot(weights, scaled_ref[...], preferred_element_type=F32)
    held[:, :share] = slot.astype(BF16)
    held[:, share:] = mass_lanes(top + jnp.log(total), held.shape[1] - share)
    for h in range(experts):
        for r in range(batches):
            at = ((lax.axis_index("expert") ^ h) * batches + (lax.axis_index("batch") ^ r)) * rows
            to = (h * (batches // 2) + r // 2) * rows
            target = send_ref if r % 2 else keep_ref
            target[to : to + rows] = held[pl.ds(pl.multiple_of(at, rows), rows)]


def merge_body(share, keep_ref, came_ref, *out_refs):
    one, two = keep_ref[...], came_ref[...]
    mass = [mass_of(p, share) for p in (one, two)]
    top = jnp.maximum(*mass)
    raised = [jnp.exp(m - top) for m in mass]
    total = raised[0] + raised[1]
    both = one[:, :share].astype(F32) * (raised[0] / total)
    both = (both + two[:, :share].astype(F32) * (raised[1] / total)).astype(BF16)
    lanes = mass_lanes(top + jnp.log(total), one.shape[1] - share)
    rows = out_refs[0].shape[0]
    for i, ref in enumerate(out_refs):
        ref[:, :share] = both[i * rows : (i + 1) * rows]
        ref[:, share:] = lanes[i * rows : (i + 1) * rows]


def slot_order(batches, experts):
    near = [(r, 0) for r in range(batches)]
    return near + [(r, h) for r in range(batches) for h in range(1, experts)]


def combine_body(width, n, experts, batches, *refs):
    part_refs, out_ref, held = refs[:n], refs[n], refs[n + 1]
    logits, _ = logits_of(*part_refs[:3], part_refs[3:], width)
    raised = jnp.exp(logits - jnp.max(logits, axis=0, keepdims=True))
    held[...] = raised / jnp.sum(raised, axis=0, keepdims=True)
    rows = logits.shape[0] // (experts * batches)
    blocks = []
    for r, h in slot_order(batches, experts):
        at = ((lax.axis_index("expert") ^ h) * batches + (lax.axis_index("batch") ^ r)) * rows
        blocks.append(held[pl.ds(pl.multiple_of(at, rows), rows)])
    out_ref[...] = jnp.concatenate(blocks, axis=0).T.astype(BF16)


def gather_body(groups, count, *refs):
    out_ref = refs[-1]
    rows, share = refs[0].shape[0], out_ref.shape[1]
    for h in range(groups):
        pieces = [refs[h * count + i][...] for i in range(count)]
        mass = [mass_of(p, share) for p in pieces]
        top = functools.reduce(jnp.maximum, mass)
        raised = [jnp.exp(m - top) for m in mass]
        total = functools.reduce(jnp.add, raised)
        out = sum(p[:, :share].astype(F32) * (w / total) for p, w in zip(pieces, raised))
        out_ref[h * rows : (h + 1) * rows] = out.astype(BF16)


def gate_up_body(s, last, *refs):
    low_ref, high_ref, gate_ref, up_ref = refs[:4]
    share = low_ref.shape[1]
    at = pl.ds(pl.multiple_of((lax.axis_index("tensor") ^ s) * share, share), share)
    x = jnp.concatenate([low_ref[...], high_ref[...]], axis=0)
    g = jnp.dot(x, gate_ref[0, at], preferred_element_type=F32)
    u = jnp.dot(x, up_ref[0, at], preferred_element_type=F32)
    if len(refs) > (5 if last else 6):
        g, u = g + refs[4][...], u + refs[5][...]
    if last:
        refs[-1][...] = (g / (1.0 + jnp.exp(-g)) * u).astype(BF16)
    else:
        refs[-2][...] = g
        refs[-1][...] = u


def down_body(s, hidden_ref, down_ref, keep_ref, send_ref):
    share = keep_ref.shape[1]
    at = pl.ds(pl.multiple_of((lax.axis_index("tensor") ^ s) * share, share), share)
    out = jnp.dot(hidden_ref[...], down_ref[0, :, at], preferred_element_type=F32).astype(BF16)
    half = out.shape[0] // 2
    keep_ref[...] = out[:half]
    send_ref[...] = out[half:]


def output_body(combine_ref, *refs):
    pieces, out_ref = refs[:-1], refs[-1]
    slots = jnp.concatenate([p[...] for p in pieces], axis=0)
    out_ref[...] = jnp.dot(combine_ref[...], slots, preferred_element_type=F32).astype(BF16)


def fetch_body(*refs):
    count = (len(refs) - 1) // 2
    copies = [
        pltpu.make_async_copy(refs[i], refs[count + i], refs[-1].at[i]) for i in range(count)
    ]
    for c in copies:
        c.start()
    for c in copies:
        c.wait()


def fetch(*arrays):
    return pl.pallas_call(
        fetch_body,
        out_shape=[pltpu.VMEM(a.shape, a.dtype) for a in arrays],
        in_specs=[pl.BlockSpec(memory_space=pltpu.HBM)] * len(arrays),
        out_specs=[VMEM] * len(arrays),
        scratch_shapes=[pltpu.SemaphoreType.DMA((len(arrays),))],
        cost_estimate=pl.CostEstimate(flops=1 << 30, bytes_accessed=1 << 25, transcendentals=0),
        compiler_params=pltpu.CompilerParams(vmem_limit_bytes=1 << 20),
        name="fetch",
    )(*(pltpu.with_memory_space_constraint(a, pltpu.HBM) for a in arrays))


def add(*xs):
    return functools.reduce(jnp.add, [x.astype(F32) for x in xs]).astype(BF16)


def local(tokens, gain, phi, w_gate, w_up, w_down):
    batches, experts, tensors = (lax.axis_size(a) for a in ("batch", "expert", "tensor"))
    for n in (batches, experts, tensors):
        assert n & (n - 1) == 0
    assert tokens.shape[0] == 1 and w_gate.shape[0] == 1
    width = w_gate.shape[1]
    token_count, share = tokens.shape[1:]
    slots = phi.shape[1]
    rows = slots // (experts * batches)

    head = 8 * max(1, (slots + 8) * HEAD // 800)
    scaled, part, first = pl.pallas_call(
        logits_body,
        out_shape=[
            shape((token_count, share), BF16),
            shape((slots + 8, token_count), F32),
            shape((head, token_count), F32),
        ],
        in_specs=[pl.BlockSpec(memory_space=pltpu.HBM)] * 3,
        out_specs=[VMEM] * 3,
        scratch_shapes=[
            pltpu.VMEM(tokens.shape, BF16),
            pltpu.VMEM(gain.shape, BF16),
            pltpu.VMEM(phi.shape, BF16),
            pltpu.SemaphoreType.DMA((3,)),
        ],
        cost_estimate=pl.CostEstimate(flops=1 << 30, bytes_accessed=1 << 22, transcendentals=0),
        compiler_params=pltpu.CompilerParams(vmem_limit_bytes=6 << 20),
        name="logits",
    )(*(pltpu.with_memory_space_constraint(x, pltpu.HBM) for x in (tokens, gain, phi)))
    near = swap(part, "tensor", 1)
    tail = part[head:] + near[head:]
    bit = 2
    while bit < tensors:
        tail = tail + swap(tail, "tensor", bit)
        bit <<= 1
    parts = [part, near, tail] + [swap(first, "tensor", s) for s in range(2, tensors)]
    parts_count = len(parts)
    half = experts * batches // 2
    keep, send = pl.pallas_call(
        functools.partial(slots_body, width, parts_count, experts, batches),
        out_shape=[shape((half * rows, share + 128), BF16)] * 2,
        in_specs=[VMEM] * (parts_count + 1),
        out_specs=[VMEM] * 2,
        scratch_shapes=[pltpu.VMEM((slots, share + 128), BF16)],
        cost_estimate=pl.CostEstimate(flops=1 << 30, bytes_accessed=1 << 22, transcendentals=0),
        compiler_params=pltpu.CompilerParams(vmem_limit_bytes=6 << 20),
        name="slots",
    )(*parts, scaled)
    messages = call(
        functools.partial(merge_body, share),
        [shape((rows, share + 128), BF16)] * half,
        keep,
        swap(send, "batch", 1),
    )
    combine = pl.pallas_call(
        functools.partial(combine_body, width, parts_count, experts, batches),
        out_shape=shape((token_count, slots), BF16),
        in_specs=[VMEM] * parts_count,
        out_specs=VMEM,
        scratch_shapes=[pltpu.VMEM((slots, token_count), F32)],
        cost_estimate=pl.CostEstimate(flops=1 << 30, bytes_accessed=1 << 22, transcendentals=0),
        compiler_params=pltpu.CompilerParams(vmem_limit_bytes=6 << 20),
        name="combine",
    )(*parts)
    count = batches // 2
    arrived = [
        m if i == 0 else swap(m, ("batch", "expert"), i % count * 2 * experts + i // count)
        for i, m in enumerate(messages)
    ]
    own = call(
        functools.partial(gather_body, experts, count),
        shape((experts * rows, share), BF16),
        *arrived,
    )
    (w_gate,) = fetch(w_gate)
    (w_up,) = fetch(w_up)
    (w_down,) = fetch(w_down)
    hidden_share = w_gate.shape[2]
    all_rows = batches * experts * rows
    carry = []
    for s in [0, 1, *range(tensors - 1, 1, -1)][:tensors]:
        piece = own if s == 0 else swap(own, "tensor", s)
        bit = batches >> 1
        while bit > 1:
            if direct(batches, s):
                other = swap(own, ("batch", "tensor"), bit * tensors + s)
            else:
                other = swap(piece, "batch", bit)
            piece = jnp.concatenate([piece, other], axis=0)
            bit >>= 1
        last = s == min(2, tensors - 1)
        carry = call(
            functools.partial(gate_up_body, s, last),
            shape((all_rows, hidden_share), BF16)
            if last
            else [shape((all_rows, hidden_share), F32)] * 2,
            piece,
            swap(piece, "batch", 1),
            w_gate,
            w_up,
            *carry,
            cost=(4 * all_rows * hidden_share * share, 1 << 24),
        )
    arrived = []
    for s in reversed(range(tensors)):
        keep, send = call(
            functools.partial(down_body, s),
            [shape((all_rows // 2, share), BF16)] * 2,
                carry,
            w_down,
            cost=(2 * all_rows * hidden_share * share, 1 << 23),
        )
        total = add(keep, swap(send, "batch", 1))
        bit = 2
        while bit < batches:
            half = total.shape[0] // 2
            other = swap(total[half:], "batch", bit)
            total = add(total[:half], other)
            bit <<= 1
        arrived.append(swap(total, "tensor", s) if s else total)
    total = add(*arrived)
    groups = [total[:rows]]
    if experts > 1:
        pieces = [swap(total[h * rows : (h + 1) * rows], "expert", h) for h in range(1, experts)]
        groups.append(jnp.concatenate(pieces, axis=0))
    gathered = []
    for group in groups:
        gathered += [group] + [swap(group, "batch", r) for r in range(1, batches)]
    cut = 2 if share % 256 == 0 else 1
    block = share // cut
    return pl.pallas_call(
        output_body,
        grid=(cut,),
        out_shape=shape((token_count, share), BF16),
        in_specs=[pl.BlockSpec(combine.shape, lambda j: (0, 0))]
        + [pl.BlockSpec((g.shape[0], block), lambda j: (0, j)) for g in gathered],
        out_specs=pl.BlockSpec((token_count, block), lambda j: (0, j)),
        compiler_params=pltpu.CompilerParams(vmem_limit_bytes=8 << 20),
        name="output",
    )(combine, *gathered)[None]


def direct(batches, s):
    return s == 1 and batches == 4


def solution(mesh):
    placed = (
        P("expert", "batch", "tensor"),
        P("tensor"),
        P("tensor", None),
        P("expert", None, ("batch", "tensor")),
        P("expert", None, ("batch", "tensor")),
        P("expert", ("batch", "tensor"), None),
    )
    return jax.shard_map(
        local, mesh=mesh, in_specs=placed, out_specs=P("expert", "batch", "tensor"), check_vma=False
    )
```
